32 devices in a mesh: grp: 2 (over x), trn: 8 (over z, y), tst: 2 (over core).
Axes of the slice: x: 2, y: 2, z: 4, core: 2. Of those that a mesh axis runs over, the one named last changes fastest.
Arguments:
- test_points: bfloat16 [64, 8192], P(None, ('grp', 'tst')), parts along dimension 1, may hold values from -9 to 9
- train_points: bfloat16 [64, 65536], P(None, ('grp', 'trn')), parts along dimension 1, may hold values from -6 to 6
- weights: bfloat16 [65536], P(('grp', 'trn')), parts along dimension 0, may hold values from -6 to 6
- factor: bfloat16 [65536, 512], P(('grp', 'trn')), parts along dimension 0, may hold values from -1.14904852 to 1.14904852
Outputs:
- mean: float32 [8192], P(('grp', 'tst')), parts along dimension 0
- variance: float32 [8192], P(('grp', 'tst')), parts along dimension 0
The draws below stay inside these ranges and needn't reach their ends.
There are 2 independent parts, one for each index of `grp`. The reference program is written for one: setup_inputs(seed, part) draws one part's arguments, and reference() takes and returns one part's arrays. A program takes and returns all parts, laid end to end along the dimension named above; each array names one. Nothing has to cross between parts.
All inputs are finite; a program needn't handle non-finite values.
Results may differ from the reference program's by a relative error of at most 0.0033.
Values sent between devices are 32-bit elements; how exact they have to be, the bound alone decides.
A program may use at most 64 MiB of HBM per device.

```python
import math
import jax
import jax.numpy as jnp
from jax import lax

DIM = 64
RANK = 512
TEST = 4096
TRAIN = 32768


def points_of(key):
    base_key = jax.random.fold_in(key, 11)
    train = jnp.clip(jax.random.normal(base_key, (DIM, TRAIN), jnp.float32), -6.0, 6.0)
    return train


def draw_train_points(key, part):
    return points_of(key).astype(jnp.bfloat16)


def draw_test_points(key, part):
    train = points_of(key)
    anchor = jax.random.randint(jax.random.fold_in(key, 12), (TEST,), 0, TRAIN)
    noise = jnp.clip(jax.random.normal(jax.random.fold_in(key, 13), (DIM, TEST), jnp.float32), -6.0, 6.0)
    spread = jnp.full((1, TEST), 0.5, jnp.float32)
    return (jnp.take(train, anchor, axis=1) + spread * noise).astype(jnp.bfloat16)


def draw_factor(key, part):
    base = jnp.clip(jax.random.normal(jax.random.fold_in(key, 21), (TRAIN, RANK), jnp.float32), -6.0, 6.0)
    return (base * (0.9 / math.sqrt(RANK))).astype(jnp.bfloat16)


def shard_levels(own_key, dims, pieces, low, high):
    def one(position, parts):
        steps = jax.random.uniform(jax.random.fold_in(jax.random.fold_in(own_key, 6), position), (parts,), jnp.float32, low / len(pieces), high / len(pieces))
        return jnp.repeat(jnp.exp(steps), dims[position] // parts).reshape((-1,) + (1,) * (len(dims) - position - 1))

    level = one(*pieces[0])
    for cut in pieces[1:]:
        level = level * one(*cut)
    return level


def normal_values(key, shape, scale, reach, split=(), kind=jnp.bfloat16):
    entries = jax.random.normal(key, shape, jnp.float32) * scale
    if len(split) > 0:
        entries = shard_levels(key, shape, split, -0.22, 0.18) * entries
    return jnp.clip(entries, min=-reach, max=reach).astype(kind)


def setup_inputs(seed: int = 0, part: int = 0) -> dict:
    streams_of = jax.random.split(jax.random.key(seed), 5)
    part_keys = jax.random.split(jax.random.fold_in(streams_of[4], part), 5)
    test_points = draw_test_points(jax.random.fold_in(jax.random.fold_in(streams_of[4], part), 71), part)
    train_points = draw_train_points(jax.random.fold_in(jax.random.fold_in(streams_of[4], part), 71), part)
    weights = normal_values(part_keys[2], (TRAIN,), 1.5, 6.0, ((0, 8),))
    factor = draw_factor(jax.random.fold_in(jax.random.fold_in(streams_of[4], part), 71), part)
    return dict(test_points=test_points, train_points=train_points, weights=weights, factor=factor)


def reference(test_points, train_points, weights, factor):
    test_sq = jnp.sum(test_points.astype(jnp.float32) ** 2, axis=0)
    total = train_points.shape[1]
    block = math.gcd(total, 1024)
    count = total // block
    width = factor.shape[1]
    rows = test_points.shape[1]

    def step(carry, index):
        mean_acc, proj_acc = carry
        start = (index * block).astype(jnp.int32)
        points = lax.dynamic_slice_in_dim(train_points, start, block, 1)
        wblock = lax.dynamic_slice_in_dim(weights, start, block, 0)
        fblock = lax.dynamic_slice_in_dim(factor, start, block, 0)
        train_sq = jnp.sum(points.astype(jnp.float32) ** 2, axis=0)
        cross = jnp.dot(test_points.T, points, preferred_element_type=jnp.float32)
        kernel = jnp.exp(-(test_sq[:, None] + train_sq[None, :] - 2.0 * cross) * (4.0 / DIM)).astype(jnp.bfloat16)
        mean_acc = mean_acc + jnp.dot(kernel, wblock, preferred_element_type=jnp.float32)
        proj_acc = proj_acc + jnp.dot(kernel, fblock, preferred_element_type=jnp.float32)
        return (mean_acc, proj_acc), None

    init = (jnp.zeros((rows,), jnp.float32), jnp.zeros((rows, width), jnp.float32))
    (mean, project), _ = lax.scan(step, init, jnp.arange(count, dtype=jnp.int32))
    variance = 1.0 - jnp.sum(project * project, axis=1)
    return mean, variance
```

```python
import functools
import math

import jax
import jax.numpy as jnp
from jax import lax
from jax.experimental import pallas as pl
from jax.experimental.pallas import tpu as pltpu
from jax.sharding import PartitionSpec as P

LOG2E = 1.4426950408889634
STEPS = 8
CHUNK = 1024
LINE = 4
LAG_Y = 3
LAG_B = (0, 3, 5, 7)
LAG_A = (0, 5, 7, 9)
LAG_X = 10


def pieces(value):
    high = value.astype(jnp.bfloat16).astype(jnp.float32)
    rest = value - high
    middle = rest.astype(jnp.bfloat16).astype(jnp.float32)
    low = (rest - middle).astype(jnp.bfloat16).astype(jnp.float32)
    return high, middle, low


def pick(row, table, default):
    value = default
    for index, entry in table:
        value = jnp.where(row == index, entry, value)
    return value


def kernel(
    test_ref, train_ref, weights_ref, factor_ref, mean_ref, var_ref,
    test_aug, train_aug, wide, part, got_y, got_br, got_bl, got_ar, got_al, got_x,
    mean_acc, var_acc, mean_box, var_box,
    s_y, r_y, s_br, r_br, s_bl, r_bl, s_ar, r_ar, s_al, r_al, s_x, r_x,
    s_mean, r_mean, s_var, r_var,
):
    count = mean_box.shape[0]
    pair = count // LINE
    last = LINE - 1
    me = lax.axis_index("trn")
    z = me // pair
    y = me % pair
    dim, rows = test_ref.shape
    local = train_ref.shape[1]
    depth = test_aug.shape[1]
    group = rows // (8 * STEPS)
    span = rows // 4
    other = z * pair + (1 - y)
    up, down = me + pair, me - pair

    barrier = pltpu.get_barrier_semaphore()

    def greet(k, carry):
        pl.semaphore_signal(barrier, inc=1, device_id={"trn": lax.rem(me + k, count)})
        return carry

    lax.fori_loop(1, count, greet, 0)

    def prepare_train(index, carry):
        cols = pl.ds(pl.multiple_of(index * 512, 512), 512)
        points = train_ref[:, cols]
        squares = points.astype(jnp.float32) ** 2
        norm = jnp.sum(squares, axis=0, keepdims=True) * (-4.0 / dim)
        high, middle, low = pieces(norm)
        row = lax.broadcasted_iota(jnp.int32, (16, 512), 0)
        one = jnp.float32(1.0)
        extra = pick(row, ((0, one), (1, one), (2, one), (3, high), (4, middle), (5, low)), jnp.float32(0.0))
        train_aug[:dim, cols] = points
        train_aug[dim : dim + 16, cols] = extra.astype(jnp.bfloat16)
        train_aug[dim + 16 :, cols] = jnp.zeros((depth - dim - 16, 512), jnp.bfloat16)
        return carry

    lax.fori_loop(0, local // 512, prepare_train, 0)
    wide[...] = weights_ref[...].astype(jnp.float32)

    def prepare_test(index, carry):
        cols = pl.ds(pl.multiple_of(index * 256, 256), 256)
        points = test_ref[:, cols].astype(jnp.float32)
        norm = jnp.sum(points * points, axis=0, keepdims=True) * (-4.0 / dim)
        high, middle, low = pieces(norm)
        row = lax.broadcasted_iota(jnp.int32, (8, 256), 0)
        one = jnp.float32(1.0)
        extra = pick(row, ((0, high), (1, middle), (2, low), (3, one), (4, one), (5, one)), jnp.float32(0.0))
        whole = jnp.concatenate(
            [points * (8.0 / dim), extra, jnp.zeros((depth - dim - 8, 256), jnp.float32)], axis=0
        )
        test_aug[cols, :] = whole.T.astype(jnp.bfloat16)
        return carry

    lax.fori_loop(0, rows // 256, prepare_test, 0)

    def row_of(owner, kind, step):
        return pl.multiple_of(owner * span + kind * (span // 2) + step * group, group)

    def places(step):
        return (
            row_of(2, 0, step), row_of(3, 0, step), row_of(0, 0, step), row_of(1, 0, step),
            row_of(1 - y, 1, step), row_of(3 - y, 1, step), row_of(y, 1, step), row_of(2 + y, 1, step),
        )

    def compute(step):
        where = places(step)
        left = jnp.concatenate([test_aug[pl.ds(at, group), :] for at in where], axis=0)
        total = None
        means = None
        for begin in range(0, local, CHUNK):
            power = jnp.dot(
                left, train_aug[:, begin : begin + CHUNK], preferred_element_type=jnp.float32
            )
            values = jnp.exp2(power * LOG2E).astype(jnp.bfloat16)
            scaled = values.astype(jnp.float32) * wide[:, begin : begin + CHUNK]
            for lane in range(0, CHUNK, 128):
                piece = scaled[:, lane : lane + 128]
                means = piece if means is None else means + piece
            product = jnp.dot(
                values, factor_ref[begin : begin + CHUNK, :], preferred_element_type=jnp.float32
            )
            total = product if total is None else total + product
        part[step] = total
        for index, at in enumerate(where):
            mean_acc[pl.ds(at, group), :] = means[index * group : (index + 1) * group, :]

    def send(source, target, ssem, rsem, device):
        return pltpu.make_async_remote_copy(
            src_ref=source, dst_ref=target, send_sem=ssem, recv_sem=rsem, device_id={"trn": device}
        )

    def copy_y(s):
        return send(part.at[s, 4 * group : 6 * group], got_y.at[s], s_y.at[s], r_y.at[s], other)

    def first_b(s, got, begin, ssem, rsem, device):
        return send(part.at[s, begin : begin + 2 * group], got.at[s], ssem.at[s], rsem.at[s], device)

    def first_a(s, got, begin, ssem, rsem, device):
        return send(part.at[s, begin : begin + group], got.at[s], ssem.at[s], rsem.at[s], device)

    def onward(s, got, ssem, rsem, device):
        return send(got.at[s], got.at[s], ssem.at[s], rsem.at[s], device)

    def swap(s, got):
        theirs = pl.ds(pl.multiple_of((1 - y) * group, group), group)
        return send(got.at[s, theirs], got_x.at[s], s_x.at[s], r_x.at[s], other)

    def square(values):
        total = None
        for lane in range(0, values.shape[1], 128):
            piece = values[:, lane : lane + 128]
            total = piece * piece if total is None else total + piece * piece
        return total

    chains_b = (
        (got_br, 0, s_br, r_br, z, up, LAG_B),
        (got_bl, 2 * group, s_bl, r_bl, last - z, down, LAG_B),
    )
    chains_a = (
        (got_ar, 7 * group, s_ar, r_ar, z, up, LAG_A),
        (got_al, 6 * group, s_al, r_al, last - z, down, LAG_A),
    )

    def lag_of(hop, table):
        value = table[1]
        for index in range(2, LINE):
            value = jnp.where(hop == index, table[index], value)
        return value

    def inside(s):
        return (s >= 0) & (s < STEPS)

    compute(0)
    pl.semaphore_wait(barrier, count - 1)

    def turn(it, carry):
        @pl.when((it > 0) & (it < STEPS))
        def _():
            compute(it)

        @pl.when(it < STEPS)
        def _():
            copy_y(it).start()
            for got, begin, ssem, rsem, hop, device, _ in chains_b:
                @pl.when(hop == 0)
                def _():
                    first_b(it, got, begin, ssem, rsem, device).start()

        for got, begin, ssem, rsem, hop, device, lags in chains_b:
            s = it - lag_of(hop, lags)

            @pl.when((hop > 0) & inside(s))
            def _():
                onward(s, got, ssem, rsem, device).wait_recv()
                got[s] = got[s] + part[s, begin : begin + 2 * group]

                @pl.when(hop < last)
                def _():
                    onward(s, got, ssem, rsem, device).start()

                @pl.when(hop == last)
                def _():
                    swap(s, got).start()

        s_here = it - LAG_Y

        @pl.when(inside(s_here))
        def _():
            copy_y(s_here).wait_recv()
            kept = slice(6 * group, 8 * group)
            part[s_here, kept] = part[s_here, kept] + got_y[s_here]
            for got, begin, ssem, rsem, hop, device, _ in chains_a:
                @pl.when(hop == 0)
                def _():
                    first_a(s_here, got, begin, ssem, rsem, device).start()

        for got, begin, ssem, rsem, hop, device, lags in chains_a:
            s = it - lag_of(hop, lags)

            @pl.when((hop > 0) & inside(s))
            def _():
                onward(s, got, ssem, rsem, device).wait_recv()

                @pl.when(hop < last)
                def _():
                    got[s] = got[s] + part[s, begin : begin + group]
                    onward(s, got, ssem, rsem, device).start()

                @pl.when(hop == last)
                def _():
                    at = pl.multiple_of(span // 2 + s * group, group)
                    var_acc[pl.ds(at, group), :] = square(got[s] + part[s, begin : begin + group])

        s_last = it - LAG_X
        for got, hop in ((got_br, z), (got_bl, last - z)):
            @pl.when((hop == last) & inside(s_last))
            def _():
                swap(s_last, got).wait_recv()
                mine = pl.ds(pl.multiple_of(y * group, group), group)
                at = pl.multiple_of(s_last * group, group)
                var_acc[pl.ds(at, group), :] = square(got[s_last, mine] + got_x[s_last])

        @pl.when(it == STEPS)
        def _():
            for index in range(rows // 128):
                block = mean_acc[index * 128 : (index + 1) * 128, :]
                mean_box[me, index : index + 1, :] = jnp.sum(block.T, axis=0, keepdims=True)

            def tell(k, carry):
                mean_copy(k).start()
                return carry

            lax.fori_loop(1, count, tell, 0)

        return carry

    def mean_copy(k):
        return send(
            mean_box.at[me], mean_box.at[me], s_mean.at[k], r_mean.at[k], lax.rem(me + k, count)
        )

    lax.fori_loop(0, STEPS + LAG_X, turn, 0)

    owner = jnp.where(z == last, 2, 0) + y
    ends = (z == 0) | (z == last)

    def var_copy(k, who):
        return send(var_box.at[who], var_box.at[who], s_var.at[k], r_var.at[who], lax.rem(me + k, count))

    @pl.when(ends)
    def _():
        for index in range(span // 128):
            block = var_acc[index * 128 : (index + 1) * 128, :]
            var_box[owner, index : index + 1, :] = 1.0 - jnp.sum(block.T, axis=0, keepdims=True)

        def tell(k, carry):
            var_copy(k, owner).start()
            return carry

        lax.fori_loop(1, count, tell, 0)

    def hear(k, carry):
        mean_copy(k).wait()
        return carry

    lax.fori_loop(1, count, hear, 0)
    total = mean_box[0]
    for index in range(1, count):
        total = total + mean_box[index]
    mean_ref[...] = total

    def settle(s, carry):
        copy_y(s).wait_send()
        for got, begin, ssem, rsem, hop, device, _ in chains_b:
            @pl.when(hop == 0)
            def _():
                first_b(s, got, begin, ssem, rsem, device).wait_send()

            @pl.when((hop > 0) & (hop < last))
            def _():
                onward(s, got, ssem, rsem, device).wait_send()

            @pl.when(hop == last)
            def _():
                swap(s, got).wait_send()

        for got, begin, ssem, rsem, hop, device, _ in chains_a:
            @pl.when(hop == 0)
            def _():
                first_a(s, got, begin, ssem, rsem, device).wait_send()

            @pl.when((hop > 0) & (hop < last))
            def _():
                onward(s, got, ssem, rsem, device).wait_send()

        return carry

    lax.fori_loop(0, STEPS, settle, 0)

    for who in range(4):
        @pl.when(jnp.logical_not(ends) | (owner != who))
        def _():
            var_copy(1, who).wait_recv()

    lines = span // 128
    for who in range(4):
        var_ref[who * lines : (who + 1) * lines, :] = var_box[who]

    @pl.when(ends)
    def _():
        def done(k, carry):
            var_copy(k, owner).wait_send()
            return carry

        lax.fori_loop(1, count, done, 0)


def fused(test_points, train_points, weights, factor, *, count):
    dim, rows = test_points.shape
    local = train_points.shape[1]
    width = factor.shape[1]
    depth = -(-(dim + 16) // 128) * 128
    group = rows // (8 * STEPS)
    dma = pltpu.SemaphoreType.DMA
    f32 = jnp.float32
    sems = [dma((STEPS,))] * 12 + [dma((count,)), dma((count,)), dma((count,)), dma((4,))]
    mean, variance = pl.pallas_call(
        kernel,
        out_shape=[jax.ShapeDtypeStruct((rows // 128, 128), f32)] * 2,
        in_specs=[pl.BlockSpec(memory_space=pltpu.VMEM)] * 4,
        out_specs=[pl.BlockSpec(memory_space=pltpu.VMEM)] * 2,
        scratch_shapes=[
            pltpu.VMEM((rows, depth), jnp.bfloat16),
            pltpu.VMEM((depth, local), jnp.bfloat16),
            pltpu.VMEM((1, local), f32),
            pltpu.VMEM((STEPS, 8 * group, width), f32),
            pltpu.VMEM((STEPS, 2 * group, width), f32),
            pltpu.VMEM((STEPS, 2 * group, width), f32),
            pltpu.VMEM((STEPS, 2 * group, width), f32),
            pltpu.VMEM((STEPS, group, width), f32),
            pltpu.VMEM((STEPS, group, width), f32),
            pltpu.VMEM((STEPS, group, width), f32),
            pltpu.VMEM((rows, 128), f32),
            pltpu.VMEM((rows // 4, 128), f32),
            pltpu.VMEM((count, rows // 128, 128), f32),
            pltpu.VMEM((4, rows // 512, 128), f32),
        ] + sems,
        compiler_params=pltpu.CompilerParams(
            collective_id=0, has_side_effects=True, vmem_limit_bytes=56 * 1024 * 1024
        ),
    )(test_points, train_points, weights.reshape(1, local), factor)
    return mean.reshape(rows), variance.reshape(rows)


def on_device(test_points, train_points, weights, factor):
    rows = test_points.shape[1]
    local = train_points.shape[1]
    dim = test_points.shape[0]
    width = factor.shape[1]
    test_sq = jnp.sum(test_points.astype(jnp.float32) ** 2, axis=0)
    block = math.gcd(local, 1024)
    turns = local // block

    def step(index, carry):
        mean_acc, proj_acc = carry
        start = (index * block).astype(jnp.int32)
        points = lax.dynamic_slice_in_dim(train_points, start, block, 1)
        wblock = lax.dynamic_slice_in_dim(weights, start, block, 0)
        fblock = lax.dynamic_slice_in_dim(factor, start, block, 0)
        train_sq = jnp.sum(points.astype(jnp.float32) ** 2, axis=0)
        cross = lax.dot_general(
            test_points, points, (((0,), (0,)), ((), ())), preferred_element_type=jnp.float32
        )
        kernel = jnp.exp(
            -(test_sq[:, None] + train_sq[None, :] - 2.0 * cross) * (4.0 / dim)
        ).astype(jnp.bfloat16)
        mean_acc = mean_acc + jnp.dot(kernel, wblock, preferred_element_type=jnp.float32)
        proj_acc = proj_acc + jnp.dot(kernel, fblock, preferred_element_type=jnp.float32)
        return (mean_acc, proj_acc)

    init = (jnp.zeros((rows,), jnp.float32), jnp.zeros((rows, width), jnp.float32))
    mean_part, proj_part = lax.fori_loop(0, turns, step, init)
    mean_share, proj_share = (
        lax.psum_scatter(mean_part, "trn", scatter_dimension=0, tiled=True),
        lax.psum_scatter(proj_part, "trn", scatter_dimension=0, tiled=True),
    )
    var_share = 1.0 - jnp.sum(proj_share * proj_share, axis=1)
    mean, variance = (
        lax.all_gather(mean_share, "trn", axis=0, tiled=True),
        lax.all_gather(var_share, "trn", axis=0, tiled=True),
    )
    return (mean, variance)


def solution(mesh):
    in_specs = (
        P(None, ("grp", "tst")),
        P(None, ("grp", "trn")),
        P(("grp", "trn")),
        P(("grp", "trn"), None),
    )
    out_specs = (P(("grp", "tst")), P(("grp", "tst")))
    count = mesh.shape["trn"]
    body = functools.partial(fused, count=count) if count == 2 * LINE else on_device
    return jax.shard_map(
        body, mesh=mesh, in_specs=in_specs, out_specs=out_specs, check_vma=False
    )
```

```python
import functools
import math

import jax
import jax.numpy as jnp
from jax import lax
from jax.experimental import pallas as pl
from jax.experimental.pallas import tpu as pltpu
from jax.sharding import PartitionSpec as P

LOG2E = 1.4426950408889634
STEPS = 16
SHARE = 4
CHUNK = 1024
LINE = 4
LAG_Y = 3
LAG_B = (0, 3, 5, 7)
LAG_A = (0, 7, 9, 11)
LAG_X = 11


def pieces(value):
    high = value.astype(jnp.bfloat16).astype(jnp.float32)
    rest = value - high
    middle = rest.astype(jnp.bfloat16).astype(jnp.float32)
    low = (rest - middle).astype(jnp.bfloat16).astype(jnp.float32)
    return high, middle, low


def pick(row, table, default):
    value = default
    for index, entry in table:
        value = jnp.where(row == index, entry, value)
    return value


def kernel(
    test_ref, train_ref, weights_ref, factor_hbm, mean_ref, var_ref,
    test_aug, train_aug, wide, part, got_y, got_br, got_bl, got_ar, got_al, got_x,
    mean_acc, var_acc, mean_box, var_box,
    s_y, r_y, s_br, r_br, s_bl, r_bl, s_ar, r_ar, s_al, r_al, s_x, r_x,
    s_mean, r_mean, s_var, r_var, factor_ref, factor_sem,
):
    count = mean_box.shape[0]
    pair = count // LINE
    last = LINE - 1
    me = lax.axis_index("trn")
    z = me // pair
    y = me % pair
    dim, rows = test_ref.shape
    local = train_ref.shape[1]
    depth = test_aug.shape[1]
    quarter = rows // (4 * STEPS)
    gb = quarter * SHARE // 8
    ga = quarter - gb
    span = rows // 4
    other = z * pair + (1 - y)
    up, down = me + pair, me - pair

    barrier = pltpu.get_barrier_semaphore()

    def greet(device):
        pl.semaphore_signal(barrier, inc=1, device_id={"trn": device})

    greet(other)
    pl.when(z < last)(lambda: greet(up))
    pl.when(z > 0)(lambda: greet(down))

    fetch = pltpu.make_async_copy(factor_hbm, factor_ref, factor_sem)
    fetch.start()

    def prepare_train(index, carry):
        cols = pl.ds(pl.multiple_of(index * 512, 512), 512)
        points = train_ref[:, cols]
        squares = points.astype(jnp.float32) ** 2
        norm = jnp.sum(squares, axis=0, keepdims=True) * (-4.0 / dim)
        high, middle, low = pieces(norm)
        row = lax.broadcasted_iota(jnp.int32, (16, 512), 0)
        one = jnp.float32(1.0)
        extra = pick(row, ((0, one), (1, one), (2, one), (3, high), (4, middle), (5, low)), jnp.float32(0.0))
        train_aug[:dim, cols] = points
        train_aug[dim : dim + 16, cols] = extra.astype(jnp.bfloat16)
        train_aug[dim + 16 :, cols] = jnp.zeros((depth - dim - 16, 512), jnp.bfloat16)
        return carry

    lax.fori_loop(0, local // 512, prepare_train, 0)
    wide[...] = weights_ref[...].astype(jnp.float32)

    def prepare_test(index, carry):
        cols = pl.ds(pl.multiple_of(index * 256, 256), 256)
        points = test_ref[:, cols].astype(jnp.float32)
        norm = jnp.sum(points * points, axis=0, keepdims=True) * (-4.0 / dim)
        high, middle, low = pieces(norm)
        row = lax.broadcasted_iota(jnp.int32, (8, 256), 0)
        one = jnp.float32(1.0)
        extra = pick(row, ((0, high), (1, middle), (2, low), (3, one), (4, one), (5, one)), jnp.float32(0.0))
        whole = jnp.concatenate(
            [points * (8.0 / dim), extra, jnp.zeros((depth - dim - 8, 256), jnp.float32)], axis=0
        )
        test_aug[cols, :] = whole.T
        return carry

    lax.fori_loop(0, rows // 256, prepare_test, 0)

    def row_of(owner, kind, step):
        inner = gb * STEPS + step * ga if kind else step * gb
        return pl.multiple_of(owner * span + inner, 8)

    def places(step):
        return (
            row_of(2, 0, step), row_of(3, 0, step), row_of(0, 0, step), row_of(1, 0, step),
            row_of(1 - y, 1, step), row_of(3 - y, 1, step), row_of(y, 1, step), row_of(2 + y, 1, step),
        )

    def compute(step):
        where = places(step)
        sizes = (gb,) * 4 + (ga,) * 4
        left = jnp.concatenate(
            [test_aug[pl.ds(at, size), :] for at, size in zip(where, sizes)], axis=0
        ).astype(jnp.bfloat16)
        total = None
        means = None
        for begin in range(0, local, CHUNK):
            power = jnp.dot(
                left, train_aug[:, begin : begin + CHUNK], preferred_element_type=jnp.float32
            )
            values = jnp.exp2(power * LOG2E).astype(jnp.bfloat16)
            scaled = values.astype(jnp.float32) * wide[:, begin : begin + CHUNK]
            for lane in range(0, CHUNK, 128):
                piece = scaled[:, lane : lane + 128]
                means = piece if means is None else means + piece
            product = jnp.dot(
                values, factor_ref[begin : begin + CHUNK, :], preferred_element_type=jnp.float32
            )
            total = product if total is None else total + product
        part[step] = total
        begin = 0
        for at, size in zip(where, sizes):
            mean_acc[pl.ds(at, size), :] = means[begin : begin + size, :]
            begin += size

    def send(source, target, ssem, rsem, device):
        return pltpu.make_async_remote_copy(
            src_ref=source, dst_ref=target, send_sem=ssem, recv_sem=rsem, device_id={"trn": device}
        )

    def copy_y(s):
        return send(part.at[s, 4 * gb : 4 * gb + 2 * ga], got_y.at[s], s_y.at[s], r_y.at[s], other)

    def first_b(s, got, begin, ssem, rsem, device):
        return send(part.at[s, begin : begin + 2 * gb], got.at[s], ssem.at[s], rsem.at[s], device)

    def first_a(s, got, begin, ssem, rsem, device):
        return send(part.at[s, begin : begin + ga], got.at[s], ssem.at[s], rsem.at[s], device)

    def onward(s, got, ssem, rsem, device):
        return send(got.at[s], got.at[s], ssem.at[s], rsem.at[s], device)

    def swap(s, got):
        theirs = pl.ds(pl.multiple_of((1 - y) * gb, 8), gb)
        return send(got.at[s, theirs], got_x.at[s], s_x.at[s], r_x.at[s], other)

    def square(values):
        total = None
        for lane in range(0, values.shape[1], 128):
            piece = values[:, lane : lane + 128]
            total = piece * piece if total is None else total + piece * piece
        return total

    chains_b = (
        (got_br, 0, s_br, r_br, z, up, LAG_B),
        (got_bl, 2 * gb, s_bl, r_bl, last - z, down, LAG_B),
    )
    chains_a = (
        (got_ar, 4 * gb + 3 * ga, s_ar, r_ar, z, up, LAG_A),
        (got_al, 4 * gb + 2 * ga, s_al, r_al, last - z, down, LAG_A),
    )

    def lag_of(hop, table):
        value = table[1]
        for index in range(2, LINE):
            value = jnp.where(hop == index, table[index], value)
        return value

    def inside(s):
        return (s >= 0) & (s < STEPS)

    fetch.wait()
    compute(0)
    between = (z > 0) & (z < last)
    pl.when(between)(lambda: pl.semaphore_wait(barrier, 3))
    pl.when(jnp.logical_not(between))(lambda: pl.semaphore_wait(barrier, 2))


    def turn(it, carry):
        @pl.when((it > 0) & (it < STEPS))
        def _():
            compute(it)

        @pl.when(it < STEPS)
        def _():
            copy_y(it).start()
            for got, begin, ssem, rsem, hop, device, _ in chains_b:
                @pl.when(hop == 0)
                def _():
                    first_b(it, got, begin, ssem, rsem, device).start()

        for got, begin, ssem, rsem, hop, device, lags in chains_b:
            s = it - lag_of(hop, lags)

            @pl.when((hop > 0) & inside(s))
            def _():
                onward(s, got, ssem, rsem, device).wait_recv()
                got[s] = got[s] + part[s, begin : begin + 2 * gb]

                @pl.when(hop < last)
                def _():
                    onward(s, got, ssem, rsem, device).start()

                @pl.when(hop == last)
                def _():
                    swap(s, got).start()

        s_here = it - LAG_Y

        @pl.when(inside(s_here))
        def _():
            copy_y(s_here).wait_recv()
            kept = slice(4 * gb + 2 * ga, 4 * gb + 4 * ga)
            part[s_here, kept] = part[s_here, kept] + got_y[s_here]
            for got, begin, ssem, rsem, hop, device, _ in chains_a:
                @pl.when(hop == 0)
                def _():
                    first_a(s_here, got, begin, ssem, rsem, device).start()

        for got, begin, ssem, rsem, hop, device, lags in chains_a:
            s = it - lag_of(hop, lags)

            @pl.when((hop > 0) & inside(s))
            def _():
                onward(s, got, ssem, rsem, device).wait_recv()

                @pl.when(hop < last)
                def _():
                    got[s] = got[s] + part[s, begin : begin + ga]
                    onward(s, got, ssem, rsem, device).start()

                @pl.when(hop == last)
                def _():
                    at = pl.multiple_of(gb * STEPS + s * ga, 8)
                    var_acc[pl.ds(at, ga), :] = square(got[s] + part[s, begin : begin + ga])

        s_last = it - LAG_X
        for got, hop in ((got_br, z), (got_bl, last - z)):
            @pl.when((hop == last) & inside(s_last))
            def _():
                swap(s_last, got).wait_recv()
                mine = pl.ds(pl.multiple_of(y * gb, 8), gb)
                at = pl.multiple_of(s_last * gb, 8)
                var_acc[pl.ds(at, gb), :] = square(got[s_last, mine] + got_x[s_last])

        @pl.when(it == STEPS + LAG_Y)
        def _():
            for index in range(rows // 128):
                block = mean_acc[index * 128 : (index + 1) * 128, :]
                mean_box[me, index : index + 1, :] = jnp.sum(block.T, axis=0, keepdims=True)

            def tell(k, carry):
                mean_copy(k).start()
                return carry

            lax.fori_loop(1, count, tell, 0)

        return carry

    def mean_copy(k):
        return send(
            mean_box.at[me], mean_box.at[me], s_mean.at[k], r_mean.at[k], lax.rem(me + k, count)
        )

    lax.fori_loop(0, STEPS + max(LAG_X, LAG_A[-1]), turn, 0)

    owner = jnp.where(z == last, 2, 0) + y
    ends = (z == 0) | (z == last)

    def var_copy(k, who):
        return send(var_box.at[who], var_box.at[who], s_var.at[k], r_var.at[who], lax.rem(me + k, count))

    @pl.when(ends)
    def _():
        for index in range(span // 128):
            block = var_acc[index * 128 : (index + 1) * 128, :]
            var_box[owner, index : index + 1, :] = 1.0 - jnp.sum(block.T, axis=0, keepdims=True)

        def tell(k, carry):
            var_copy(k, owner).start()
            return carry

        lax.fori_loop(1, count, tell, 0)

    def hear(k, carry):
        mean_copy(k).wait()
        return carry

    lax.fori_loop(1, count, hear, 0)
    total = mean_box[0]
    for index in range(1, count):
        total = total + mean_box[index]
    mean_ref[...] = total

    def settle(s, carry):
        copy_y(s).wait_send()
        for got, begin, ssem, rsem, hop, device, _ in chains_b:
            @pl.when(hop == 0)
            def _():
                first_b(s, got, begin, ssem, rsem, device).wait_send()

            @pl.when((hop > 0) & (hop < last))
            def _():
                onward(s, got, ssem, rsem, device).wait_send()

            @pl.when(hop == last)
            def _():
                swap(s, got).wait_send()

        for got, begin, ssem, rsem, hop, device, _ in chains_a:
            @pl.when(hop == 0)
            def _():
                first_a(s, got, begin, ssem, rsem, device).wait_send()

            @pl.when((hop > 0) & (hop < last))
            def _():
                onward(s, got, ssem, rsem, device).wait_send()

        return carry

    lax.fori_loop(0, STEPS, settle, 0)

    for who in range(4):
        @pl.when(jnp.logical_not(ends) | (owner != who))
        def _():
            var_copy(1, who).wait_recv()

    lines = span // 128
    for who in range(4):
        var_ref[who * lines : (who + 1) * lines, :] = var_box[who]

    @pl.when(ends)
    def _():
        def done(k, carry):
            var_copy(k, owner).wait_send()
            return carry

        lax.fori_loop(1, count, done, 0)


def fused(test_points, train_points, weights, factor, *, count):
    dim, rows = test_points.shape
    local = train_points.shape[1]
    width = factor.shape[1]
    depth = -(-(dim + 16) // 128) * 128
    quarter = rows // (4 * STEPS)
    gb = quarter * SHARE // 8
    ga = quarter - gb
    dma = pltpu.SemaphoreType.DMA
    f32 = jnp.float32
    sems = [dma((STEPS,))] * 12 + [dma((count,)), dma((count,)), dma((count,)), dma((4,))]
    mean, variance = pl.pallas_call(
        kernel,
        out_shape=[jax.ShapeDtypeStruct((rows // 128, 128), f32)] * 2,
        in_specs=[pl.BlockSpec(memory_space=pltpu.VMEM)] * 3
        + [pl.BlockSpec(memory_space=pl.ANY)],
        out_specs=[pl.BlockSpec(memory_space=pltpu.VMEM)] * 2,
        scratch_shapes=[
            pltpu.VMEM((rows, depth), f32),
            pltpu.VMEM((depth, local), jnp.bfloat16),
            pltpu.VMEM((1, local), f32),
            pltpu.VMEM((STEPS, 4 * quarter, width), f32),
            pltpu.VMEM((STEPS, 2 * ga, width), f32),
            pltpu.VMEM((STEPS, 2 * gb, width), f32),
            pltpu.VMEM((STEPS, 2 * gb, width), f32),
            pltpu.VMEM((STEPS, ga, width), f32),
            pltpu.VMEM((STEPS, ga, width), f32),
            pltpu.VMEM((STEPS, gb, width), f32),
            pltpu.VMEM((rows, 128), f32),
            pltpu.VMEM((rows // 4, 128), f32),
            pltpu.VMEM((count, rows // 128, 128), f32),
            pltpu.VMEM((4, rows // 512, 128), f32),
        ] + sems + [pltpu.VMEM((local, width), jnp.bfloat16), dma],
        compiler_params=pltpu.CompilerParams(
            collective_id=0, has_side_effects=True, vmem_limit_bytes=56 * 1024 * 1024
        ),
    )(test_points, train_points, weights.reshape(1, local), factor)
    return mean.reshape(rows), variance.reshape(rows)


def on_device(test_points, train_points, weights, factor):
    rows = test_points.shape[1]
    local = train_points.shape[1]
    dim = test_points.shape[0]
    width = factor.shape[1]
    test_sq = jnp.sum(test_points.astype(jnp.float32) ** 2, axis=0)
    block = math.gcd(local, 1024)
    turns = local // block

    def step(index, carry):
        mean_acc, proj_acc = carry
        start = (index * block).astype(jnp.int32)
        points = lax.dynamic_slice_in_dim(train_points, start, block, 1)
        wblock = lax.dynamic_slice_in_dim(weights, start, block, 0)
        fblock = lax.dynamic_slice_in_dim(factor, start, block, 0)
        train_sq = jnp.sum(points.astype(jnp.float32) ** 2, axis=0)
        cross = lax.dot_general(
            test_points, points, (((0,), (0,)), ((), ())), preferred_element_type=jnp.float32
        )
        kernel = jnp.exp(
            -(test_sq[:, None] + train_sq[None, :] - 2.0 * cross) * (4.0 / dim)
        ).astype(jnp.bfloat16)
        mean_acc = mean_acc + jnp.dot(kernel, wblock, preferred_element_type=jnp.float32)
        proj_acc = proj_acc + jnp.dot(kernel, fblock, preferred_element_type=jnp.float32)
        return (mean_acc, proj_acc)

    init = (jnp.zeros((rows,), jnp.float32), jnp.zeros((rows, width), jnp.float32))
    mean_part, proj_part = lax.fori_loop(0, turns, step, init)
    mean_share, proj_share = (
        lax.psum_scatter(mean_part, "trn", scatter_dimension=0, tiled=True),
        lax.psum_scatter(proj_part, "trn", scatter_dimension=0, tiled=True),
    )
    var_share = 1.0 - jnp.sum(proj_share * proj_share, axis=1)
    mean, variance = (
        lax.all_gather(mean_share, "trn", axis=0, tiled=True),
        lax.all_gather(var_share, "trn", axis=0, tiled=True),
    )
    return (mean, variance)


def solution(mesh):
    in_specs = (
        P(None, ("grp", "tst")),
        P(None, ("grp", "trn")),
        P(("grp", "trn")),
        P(("grp", "trn"), None),
    )
    out_specs = (P(("grp", "tst")), P(("grp", "tst")))
    count = mesh.shape["trn"]
    body = functools.partial(fused, count=count) if count == 2 * LINE else on_device
    return jax.shard_map(
        body, mesh=mesh, in_specs=in_specs, out_specs=out_specs, check_vma=False
    )
```

```python
import functools
import math

import jax
import jax.numpy as jnp
from jax import lax
from jax.experimental import pallas as pl
from jax.experimental.pallas import tpu as pltpu
from jax.sharding import PartitionSpec as P

LOG2E = 1.4426950408889634
STEPS = 16
SHARE = 4
CHUNK = 1024
LINE = 4
LAG_Y = 3
LAG_B = (0, 3, 5, 7)
LAG_A = (0, 7, 9, 11)
LAG_X = 11


def pieces(value):
    high = value.astype(jnp.bfloat16).astype(jnp.float32)
    rest = value - high
    middle = rest.astype(jnp.bfloat16).astype(jnp.float32)
    low = (rest - middle).astype(jnp.bfloat16).astype(jnp.float32)
    return high, middle, low


def pick(row, table, default):
    value = default
    for index, entry in table:
        value = jnp.where(row == index, entry, value)
    return value


def kernel(
    test_ref, train_ref, weights_ref, factor_hbm, out_ref,
    test_aug, train_aug, wide, part, got_y, got_br, got_bl, got_ar, got_al, got_x,
    mean_acc, var_acc, mean_box, var_box,
    s_y, r_y, s_br, r_br, s_bl, r_bl, s_ar, r_ar, s_al, r_al, s_x, r_x,
    s_mean, r_mean, s_var, r_var, factor_ref, factor_sem,
):
    count = mean_box.shape[0]
    pair = count // LINE
    last = LINE - 1
    me = lax.axis_index("trn")
    z = me // pair
    y = me % pair
    dim, rows = test_ref.shape
    local = train_ref.shape[1]
    depth = test_aug.shape[1]
    quarter = rows // (4 * STEPS)
    gb = quarter * SHARE // 8
    ga = quarter - gb
    span = rows // 4
    other = z * pair + (1 - y)
    up, down = me + pair, me - pair

    barrier = pltpu.get_barrier_semaphore()

    def greet(device):
        pl.semaphore_signal(barrier, inc=1, device_id={"trn": device})

    greet(other)
    pl.when(z < last)(lambda: greet(up))
    pl.when(z > 0)(lambda: greet(down))

    fetch = pltpu.make_async_copy(factor_hbm, factor_ref, factor_sem)
    fetch.start()

    def prepare_train(index, carry):
        cols = pl.ds(pl.multiple_of(index * 512, 512), 512)
        points = train_ref[:, cols]
        squares = points.astype(jnp.float32) ** 2
        norm = jnp.sum(squares, axis=0, keepdims=True) * (-4.0 / dim)
        high, middle, low = pieces(norm)
        row = lax.broadcasted_iota(jnp.int32, (16, 512), 0)
        one = jnp.float32(1.0)
        extra = pick(row, ((0, one), (1, one), (2, one), (3, high), (4, middle), (5, low)), jnp.float32(0.0))
        train_aug[:dim, cols] = points
        train_aug[dim : dim + 16, cols] = extra.astype(jnp.bfloat16)
        train_aug[dim + 16 :, cols] = jnp.zeros((depth - dim - 16, 512), jnp.bfloat16)
        return carry

    lax.fori_loop(0, local // 512, prepare_train, 0)
    wide[...] = weights_ref[...].astype(jnp.float32)

    def prepare_test(index, carry):
        cols = pl.ds(pl.multiple_of(index * 256, 256), 256)
        points = test_ref[:, cols].astype(jnp.float32)
        norm = jnp.sum(points * points, axis=0, keepdims=True) * (-4.0 / dim)
        high, middle, low = pieces(norm)
        row = lax.broadcasted_iota(jnp.int32, (8, 256), 0)
        one = jnp.float32(1.0)
        extra = pick(row, ((0, high), (1, middle), (2, low), (3, one), (4, one), (5, one)), jnp.float32(0.0))
        whole = jnp.concatenate(
            [points * (8.0 / dim), extra, jnp.zeros((depth - dim - 8, 256), jnp.float32)], axis=0
        )
        test_aug[cols, :] = whole.T
        return carry

    lax.fori_loop(0, rows // 256, prepare_test, 0)

    def row_of(owner, kind, step):
        inner = gb * STEPS + step * ga if kind else step * gb
        return pl.multiple_of(owner * span + inner, 8)

    def places(step):
        return (
            row_of(2, 0, step), row_of(3, 0, step), row_of(0, 0, step), row_of(1, 0, step),
            row_of(1 - y, 1, step), row_of(3 - y, 1, step), row_of(y, 1, step), row_of(2 + y, 1, step),
        )

    def compute(step):
        where = places(step)
        sizes = (gb,) * 4 + (ga,) * 4
        left = jnp.concatenate(
            [test_aug[pl.ds(at, size), :] for at, size in zip(where, sizes)], axis=0
        ).astype(jnp.bfloat16)
        total = None
        means = None
        for begin in range(0, local, CHUNK):
            power = jnp.dot(
                left, train_aug[:, begin : begin + CHUNK], preferred_element_type=jnp.float32
            )
            values = jnp.exp2(power * LOG2E).astype(jnp.bfloat16)
            scaled = values.astype(jnp.float32) * wide[:, begin : begin + CHUNK]
            for lane in range(0, CHUNK, 128):
                piece = scaled[:, lane : lane + 128]
                means = piece if means is None else means + piece
            product = jnp.dot(
                values, factor_ref[begin : begin + CHUNK, :], preferred_element_type=jnp.float32
            )
            total = product if total is None else total + product
        part[step] = total
        begin = 0
        for at, size in zip(where, sizes):
            mean_acc[pl.ds(at, size), :] = means[begin : begin + size, :]
            begin += size

    def send(source, target, ssem, rsem, device):
        return pltpu.make_async_remote_copy(
            src_ref=source, dst_ref=target, send_sem=ssem, recv_sem=rsem, device_id={"trn": device}
        )

    def copy_y(s):
        return send(part.at[s, 4 * gb : 4 * gb + 2 * ga], got_y.at[s], s_y.at[s], r_y.at[s], other)

    def first_b(s, got, begin, ssem, rsem, device):
        return send(part.at[s, begin : begin + 2 * gb], got.at[s], ssem.at[s], rsem.at[s], device)

    def first_a(s, got, begin, ssem, rsem, device):
        return send(part.at[s, begin : begin + ga], got.at[s], ssem.at[s], rsem.at[s], device)

    def onward(s, got, ssem, rsem, device):
        return send(got.at[s], got.at[s], ssem.at[s], rsem.at[s], device)

    def swap(s, got):
        theirs = pl.ds(pl.multiple_of((1 - y) * gb, 8), gb)
        return send(got.at[s, theirs], got_x.at[s], s_x.at[s], r_x.at[s], other)

    def square(values):
        total = None
        for lane in range(0, values.shape[1], 128):
            piece = values[:, lane : lane + 128]
            total = piece * piece if total is None else total + piece * piece
        return total

    chains_b = (
        (got_br, 0, s_br, r_br, z, up, LAG_B),
        (got_bl, 2 * gb, s_bl, r_bl, last - z, down, LAG_B),
    )
    chains_a = (
        (got_ar, 4 * gb + 3 * ga, s_ar, r_ar, z, up, LAG_A),
        (got_al, 4 * gb + 2 * ga, s_al, r_al, last - z, down, LAG_A),
    )

    def lag_of(hop, table):
        value = table[1]
        for index in range(2, LINE):
            value = jnp.where(hop == index, table[index], value)
        return value

    def inside(s):
        return (s >= 0) & (s < STEPS)

    fetch.wait()
    compute(0)
    between = (z > 0) & (z < last)
    pl.when(between)(lambda: pl.semaphore_wait(barrier, 3))
    pl.when(jnp.logical_not(between))(lambda: pl.semaphore_wait(barrier, 2))


    def turn(it, carry):
        @pl.when((it > 0) & (it < STEPS))
        def _():
            compute(it)

        @pl.when(it < STEPS)
        def _():
            copy_y(it).start()
            for got, begin, ssem, rsem, hop, device, _ in chains_b:
                @pl.when(hop == 0)
                def _():
                    first_b(it, got, begin, ssem, rsem, device).start()

        for got, begin, ssem, rsem, hop, device, lags in chains_b:
            s = it - lag_of(hop, lags)

            @pl.when((hop > 0) & inside(s))
            def _():
                onward(s, got, ssem, rsem, device).wait_recv()
                got[s] = got[s] + part[s, begin : begin + 2 * gb]

                @pl.when(hop < last)
                def _():
                    onward(s, got, ssem, rsem, device).start()

                @pl.when(hop == last)
                def _():
                    swap(s, got).start()

        s_here = it - LAG_Y

        @pl.when(inside(s_here))
        def _():
            copy_y(s_here).wait_recv()
            kept = slice(4 * gb + 2 * ga, 4 * gb + 4 * ga)
            part[s_here, kept] = part[s_here, kept] + got_y[s_here]
            for got, begin, ssem, rsem, hop, device, _ in chains_a:
                @pl.when(hop == 0)
                def _():
                    first_a(s_here, got, begin, ssem, rsem, device).start()

        for got, begin, ssem, rsem, hop, device, lags in chains_a:
            s = it - lag_of(hop, lags)

            @pl.when((hop > 0) & inside(s))
            def _():
                onward(s, got, ssem, rsem, device).wait_recv()

                @pl.when(hop < last)
                def _():
                    got[s] = got[s] + part[s, begin : begin + ga]
                    onward(s, got, ssem, rsem, device).start()

                @pl.when(hop == last)
                def _():
                    at = pl.multiple_of(gb * STEPS + s * ga, 8)
                    var_acc[pl.ds(at, ga), :] = square(got[s] + part[s, begin : begin + ga])

        s_last = it - LAG_X
        for got, hop in ((got_br, z), (got_bl, last - z)):
            @pl.when((hop == last) & inside(s_last))
            def _():
                swap(s_last, got).wait_recv()
                mine = pl.ds(pl.multiple_of(y * gb, 8), gb)
                at = pl.multiple_of(s_last * gb, 8)
                var_acc[pl.ds(at, gb), :] = square(got[s_last, mine] + got_x[s_last])

        @pl.when(it == STEPS + LAG_Y)
        def _():
            for index in range(rows // 128):
                block = mean_acc[index * 128 : (index + 1) * 128, :]
                mean_box[me, index : index + 1, :] = jnp.sum(block.T, axis=0, keepdims=True)

            def tell(k, carry):
                mean_copy(k).start()
                return carry

            lax.fori_loop(1, count, tell, 0)

        return carry

    def mean_copy(k):
        return send(
            mean_box.at[me], mean_box.at[me], s_mean.at[k], r_mean.at[k], lax.rem(me + k, count)
        )

    lax.fori_loop(0, STEPS + max(LAG_X, LAG_A[-1]), turn, 0)

    owner = jnp.where(z == last, 2, 0) + y
    ends = (z == 0) | (z == last)

    def var_copy(k, who):
        return send(var_box.at[who], var_box.at[who], s_var.at[k], r_var.at[who], lax.rem(me + k, count))

    @pl.when(ends)
    def _():
        for index in range(span // 128):
            block = var_acc[index * 128 : (index + 1) * 128, :]
            var_box[owner, index : index + 1, :] = 1.0 - jnp.sum(block.T, axis=0, keepdims=True)

        def tell(k, carry):
            var_copy(k, owner).start()
            return carry

        lax.fori_loop(1, count, tell, 0)

    def hear(k, carry):
        mean_copy(k).wait()
        return carry

    lax.fori_loop(1, count, hear, 0)
    total = mean_box[0]
    for index in range(1, count):
        total = total + mean_box[index]
    out_ref[: rows // 128, :] = total

    def settle(s, carry):
        copy_y(s).wait_send()
        for got, begin, ssem, rsem, hop, device, _ in chains_b:
            @pl.when(hop == 0)
            def _():
                first_b(s, got, begin, ssem, rsem, device).wait_send()

            @pl.when((hop > 0) & (hop < last))
            def _():
                onward(s, got, ssem, rsem, device).wait_send()

            @pl.when(hop == last)
            def _():
                swap(s, got).wait_send()

        for got, begin, ssem, rsem, hop, device, _ in chains_a:
            @pl.when(hop == 0)
            def _():
                first_a(s, got, begin, ssem, rsem, device).wait_send()

            @pl.when((hop > 0) & (hop < last))
            def _():
                onward(s, got, ssem, rsem, device).wait_send()

        return carry

    lax.fori_loop(0, STEPS, settle, 0)

    for who in range(4):
        @pl.when(jnp.logical_not(ends) | (owner != who))
        def _():
            var_copy(1, who).wait_recv()

    lines = span // 128
    for who in range(4):
        begin = rows // 128 + who * lines
        out_ref[begin : begin + lines, :] = var_box[who]

    @pl.when(ends)
    def _():
        def done(k, carry):
            var_copy(k, owner).wait_send()
            return carry

        lax.fori_loop(1, count, done, 0)


def fused(test_points, train_points, weights, factor, *, count):
    dim, rows = test_points.shape
    local = train_points.shape[1]
    width = factor.shape[1]
    depth = -(-(dim + 16) // 128) * 128
    quarter = rows // (4 * STEPS)
    gb = quarter * SHARE // 8
    ga = quarter - gb
    dma = pltpu.SemaphoreType.DMA
    f32 = jnp.float32
    sems = [dma((STEPS,))] * 12 + [dma((count,)), dma((count,)), dma((count,)), dma((4,))]
    out = pl.pallas_call(
        kernel,
        out_shape=jax.ShapeDtypeStruct((rows // 64, 128), f32),
        in_specs=[pl.BlockSpec(memory_space=pltpu.VMEM)] * 3
        + [pl.BlockSpec(memory_space=pl.ANY)],
        out_specs=pl.BlockSpec(memory_space=pltpu.VMEM),
        scratch_shapes=[
            pltpu.VMEM((rows, depth), f32),
            pltpu.VMEM((depth, local), jnp.bfloat16),
            pltpu.VMEM((1, local), f32),
            pltpu.VMEM((STEPS, 4 * quarter, width), f32),
            pltpu.VMEM((STEPS, 2 * ga, width), f32),
            pltpu.VMEM((STEPS, 2 * gb, width), f32),
            pltpu.VMEM((STEPS, 2 * gb, width), f32),
            pltpu.VMEM((STEPS, ga, width), f32),
            pltpu.VMEM((STEPS, ga, width), f32),
            pltpu.VMEM((STEPS, gb, width), f32),
            pltpu.VMEM((rows, 128), f32),
            pltpu.VMEM((rows // 4, 128), f32),
            pltpu.VMEM((count, rows // 128, 128), f32),
            pltpu.VMEM((4, rows // 512, 128), f32),
        ] + sems + [pltpu.VMEM((local, width), jnp.bfloat16), dma],
        compiler_params=pltpu.CompilerParams(
            collective_id=0, has_side_effects=True, vmem_limit_bytes=56 * 1024 * 1024
        ),
    )(test_points, train_points, weights.reshape(1, local), factor)
    lines = rows // 128
    return out[:lines].reshape(rows), out[lines:].reshape(rows)


def on_device(test_points, train_points, weights, factor):
    rows = test_points.shape[1]
    local = train_points.shape[1]
    dim = test_points.shape[0]
    width = factor.shape[1]
    test_sq = jnp.sum(test_points.astype(jnp.float32) ** 2, axis=0)
    block = math.gcd(local, 1024)
    turns = local // block

    def step(index, carry):
        mean_acc, proj_acc = carry
        start = (index * block).astype(jnp.int32)
        points = lax.dynamic_slice_in_dim(train_points, start, block, 1)
        wblock = lax.dynamic_slice_in_dim(weights, start, block, 0)
        fblock = lax.dynamic_slice_in_dim(factor, start, block, 0)
        train_sq = jnp.sum(points.astype(jnp.float32) ** 2, axis=0)
        cross = lax.dot_general(
            test_points, points, (((0,), (0,)), ((), ())), preferred_element_type=jnp.float32
        )
        kernel = jnp.exp(
            -(test_sq[:, None] + train_sq[None, :] - 2.0 * cross) * (4.0 / dim)
        ).astype(jnp.bfloat16)
        mean_acc = mean_acc + jnp.dot(kernel, wblock, preferred_element_type=jnp.float32)
        proj_acc = proj_acc + jnp.dot(kernel, fblock, preferred_element_type=jnp.float32)
        return (mean_acc, proj_acc)

    init = (jnp.zeros((rows,), jnp.float32), jnp.zeros((rows, width), jnp.float32))
    mean_part, proj_part = lax.fori_loop(0, turns, step, init)
    mean_share, proj_share = (
        lax.psum_scatter(mean_part, "trn", scatter_dimension=0, tiled=True),
        lax.psum_scatter(proj_part, "trn", scatter_dimension=0, tiled=True),
    )
    var_share = 1.0 - jnp.sum(proj_share * proj_share, axis=1)
    mean, variance = (
        lax.all_gather(mean_share, "trn", axis=0, tiled=True),
        lax.all_gather(var_share, "trn", axis=0, tiled=True),
    )
    return (mean, variance)


def solution(mesh):
    in_specs = (
        P(None, ("grp", "tst")),
        P(None, ("grp", "trn")),
        P(("grp", "trn")),
        P(("grp", "trn"), None),
    )
    out_specs = (P(("grp", "tst")), P(("grp", "tst")))
    count = mesh.shape["trn"]
    body = functools.partial(fused, count=count) if count == 2 * LINE else on_device
    return jax.shard_map(
        body, mesh=mesh, in_specs=in_specs, out_specs=out_specs, check_vma=False
    )
```
